128 devices in a mesh: dom: 128 (over y, x, z, core).
Axes of the slice: x: 4, y: 4, z: 4, core: 2. Of those that a mesh axis runs over, the one named last changes fastest.
Arguments:
- z_state: bfloat16 [96, 1048576], P(None, 'dom'), may hold values from 0 to 20, as said below
- inputs: bfloat16 [128, 1048576], P(None, 'dom'), may hold values from -6 to 6
- adjoint: bfloat16 [96, 1048576], P(None, 'dom'), may hold values from -6 to 6
- cotangent: bfloat16 [96, 1048576], P(None, 'dom'), may hold values from -0.59765625 to 0.59765625
- mix_weight: bfloat16 [96, 96], replicated, may hold values from -0.625 to 0.625
- input_weight: bfloat16 [96, 128], replicated, may hold values from -0.5 to 0.5
- tile_values: bfloat16 [32768, 128, 128], P('dom'), may hold values from 0 to 0.019897461
- tile_src: int32 [128, 256], P('dom'), may hold values from 0 to 191, as said below
- tile_dst: int32 [128, 256], P('dom'), may hold values from 0 to 63
- send_list: int32 [128, 8, 16], P('dom'), may hold values from 0 to 63
Outputs:
- fixed_next: bfloat16 [96, 1048576], P(None, 'dom')
- adjoint_next: bfloat16 [96, 1048576], P(None, 'dom')
- weight_grad: float32 [96, 96], replicated
- input_grad: float32 [96, 128], replicated
The draws below stay inside these ranges and needn't reach their ends.
Inputs may be any that keep to these rules, and one draw needn't show every extreme that they name: `tile_src`: codes below 64 name a local tile; code 64 + o * 16 + c names slot c of neighbour o's list for this partition. Every code from 64 upward appears on every partition. `z_state`: zero or positive; a state after a rectifier.
All inputs are finite; a program needn't handle non-finite values.
Results may differ from the reference program's by a relative error of at most 0.0058.
Values may be sent and summed in bfloat16 or wider, within the bound.
No kernel may reach another device: no remote copies, remote signals or barrier semaphores. Data moves between devices by JAX's collectives and lax.ppermute only.
A program may use at most 128 MiB of HBM per device.

```python
import math
import jax
import jax.numpy as jnp
from jax import lax

H = 96
F = 128
NODE_DEV = 8192
TILE = 128
REACH = 4
TILES_LOC = 64
CAP = 16
TILES_DEV = 256
NODES = 1048576
TILES = 32768
N_DOM = 128


def draw_z_state(key, part):
    noise_key = jax.random.fold_in(jax.random.fold_in(key, 5), 0)
    values = jax.random.normal(noise_key, (H, NODES), jnp.float32)
    return jnp.maximum(values, 0.0).astype(jnp.bfloat16)


def draw_tile_src(key, part):
    local_tiles = NODE_DEV // TILE
    remote = 2 * REACH * CAP

    def one_device(device_key):
        fill_key, order_key = jax.random.split(device_key)
        fixed_codes = local_tiles + jnp.arange(remote, dtype=jnp.int32)
        further = jax.random.randint(fill_key, (TILES_DEV - remote,), 0, local_tiles + remote, dtype=jnp.int32)
        return jax.random.permutation(order_key, jnp.concatenate([fixed_codes, further]))
    device_keys = jax.random.split(jax.random.fold_in(key, 11), N_DOM)
    return jax.vmap(one_device)(device_keys)


def with_ends(drawn, own_key, low, largest):
    extent = drawn.shape
    index_at = [jax.random.randint(jax.random.fold_in(own_key, axis), (), 0, extent[axis]) for axis in range(len(extent))]
    drawn = drawn.at[tuple(index_at)].set(low)
    longest = extent.index(max(extent))
    index_at[longest] = (index_at[longest] + 1) % extent[longest]
    return drawn.at[tuple(index_at)].set(largest)


def block_scale(stream_key, shape, cuts, least, top_value):
    loudness, own = 1.0, jax.random.fold_in(stream_key, 6)
    for axis_at, parts in cuts:
        steps = jnp.exp(jax.random.uniform(jax.random.fold_in(own, axis_at), (parts,), jnp.float32, least / len(cuts), top_value / len(cuts)))
        loudness = loudness * jnp.repeat(steps, shape[axis_at] // parts).reshape([-1 if axis == axis_at else 1 for axis in range(len(shape))])
    return loudness


def scatter_about(own_key, shape, scale, reach, cuts=(), kind=jnp.bfloat16):
    level = block_scale(own_key, shape, cuts, -0.22, 0.18) if cuts else 1.0
    array = jax.random.normal(own_key, shape, jnp.float32) * scale * level
    return jnp.minimum(jnp.maximum(array, -reach), reach).astype(kind)


def setup_inputs(seed: int = 0) -> dict:
    key_list = jax.random.split(jax.random.key(seed), 11)
    return {
        "z_state": draw_z_state(jax.random.fold_in(key_list[10], 71), 0),
        "inputs": scatter_about(key_list[1], (F, NODES), 1.0, 6.0, ((1, 128),)),
        "adjoint": scatter_about(key_list[2], (H, NODES), 1.0, 6.0, ((1, 128),)),
        "cotangent": scatter_about(key_list[3], (H, NODES), 0.1, 0.59765625, ((1, 128),)),
        "mix_weight": scatter_about(key_list[4], (H, H), H ** -0.5, 0.625),
        "input_weight": scatter_about(key_list[5], (H, F), F ** -0.5, 0.5),
        "tile_values": jnp.clip(0.019897461 * jax.random.uniform(key_list[6], (TILES, TILE, TILE), jnp.float32) ** block_scale(key_list[6], (TILES, TILE, TILE), ((0, 128),), -0.2, 0.2), 0.0, 0.019897461).astype(jnp.bfloat16),
        "tile_src": draw_tile_src(jax.random.fold_in(key_list[10], 71), 0),
        "tile_dst": with_ends(jax.random.randint(key_list[8], (N_DOM, TILES_DEV), 0, TILES_LOC), jax.random.fold_in(key_list[8], 1), 0, TILES_LOC - 1).astype(jnp.int32),
        "send_list": with_ends(jax.random.randint(key_list[9], (N_DOM, 2 * REACH, CAP), 0, TILES_LOC), jax.random.fold_in(key_list[9], 1), 0, TILES_LOC - 1).astype(jnp.int32),
    }


highest = lax.Precision.HIGHEST

def peer_offsets():
    index = jnp.arange(2 * REACH, dtype=jnp.int32)
    return jnp.where(index < REACH, index + 1, REACH - 1 - index).astype(jnp.int32)

def global_sources(send_list, tile_src):
    devices = jnp.arange(N_DOM, dtype=jnp.int32)[:, None]
    remote = jnp.maximum(tile_src - TILES_LOC, 0).astype(jnp.int32)
    offset_index = (remote // CAP).astype(jnp.int32)
    slot_column = (remote % CAP).astype(jnp.int32)
    peer_device = ((devices - peer_offsets()[offset_index]) % N_DOM).astype(jnp.int32)
    far_tiles = peer_device * TILES_LOC + send_list[peer_device, offset_index, slot_column]
    near_tiles = devices * TILES_LOC + tile_src
    return jnp.where(tile_src < TILES_LOC, near_tiles, far_tiles).astype(jnp.int32)

def reference(z_state, inputs, adjoint, cotangent, mix_weight, input_weight, tile_values, tile_src, tile_dst, send_list):
    sources = global_sources(send_list, tile_src)
    blocks = tile_values.reshape(N_DOM, TILES_DEV, TILE, TILE)
    state_tiles = z_state.reshape(H, N_DOM * TILES_LOC, TILE)

    def forward_device(operands):
        source_ids, dest_ids, device_blocks = operands
        pieces = state_tiles[:, source_ids].astype(jnp.float32)
        contributions = jnp.einsum('hks,ksd->khd', pieces, device_blocks.astype(jnp.float32), precision=highest)
        return jax.ops.segment_sum(contributions, dest_ids, TILES_LOC)
    gathered = lax.map(forward_device, (sources, tile_dst, blocks))
    aggregated = jnp.moveaxis(gathered, 2, 0).reshape(H, NODES).astype(jnp.bfloat16)
    preactivation = jnp.dot(mix_weight, aggregated, preferred_element_type=jnp.float32) + jnp.dot(input_weight, inputs, preferred_element_type=jnp.float32)
    fixed_next = jnp.maximum(preactivation, 0.0).astype(jnp.bfloat16)
    masked = jnp.where(z_state > 0, adjoint, jnp.zeros_like(adjoint))
    backward = jnp.dot(mix_weight.T, masked, preferred_element_type=jnp.float32).astype(jnp.bfloat16)
    back_tiles = backward.reshape(H, N_DOM * TILES_LOC, TILE)

    def backward_device(running, operands):
        device, source_ids, dest_ids, device_blocks = operands
        pieces = back_tiles[:, device * TILES_LOC + dest_ids].astype(jnp.float32)
        partials = jnp.einsum('hkd,ksd->khs', pieces, device_blocks.astype(jnp.float32), precision=highest)
        return (running.at[source_ids].add(partials), None)
    start = jnp.zeros((N_DOM * TILES_LOC, H, TILE), jnp.float32)
    device_ids = jnp.arange(N_DOM, dtype=jnp.int32)
    summed, unused = lax.scan(backward_device, start, (device_ids, sources, tile_dst, blocks))
    adjoint_sum = jnp.moveaxis(summed, 1, 0).reshape(H, NODES)
    adjoint_next = (cotangent.astype(jnp.float32) + adjoint_sum).astype(jnp.bfloat16)
    normalizer = 1.0 / math.sqrt(NODES)
    weight_grad = jnp.dot(masked, aggregated.T, preferred_element_type=jnp.float32) * normalizer
    input_grad = jnp.dot(masked, inputs.T, preferred_element_type=jnp.float32) * normalizer
    return (fixed_next, adjoint_next, weight_grad, input_grad)
```

```python
import math

import jax
import jax.numpy as jnp
from jax import lax
from jax.experimental import pallas as pl
from jax.experimental.pallas import tpu as pltpu
from jax.sharding import PartitionSpec as P


AXIS = "dom"
H = 96
F = 128
T = 128
LOC = 64
CAP = 16
PEERS = 8
TILES = 256
NODES_DEV = LOC * T
CODES = LOC + PEERS * CAP
CHUNKS = 8
PER = TILES // CHUNKS
UNROLL = 8
OFFSETS = (1, 2, 3, 4, -1, -2, -3, -4)
ORDER = (7, 3, 6, 2, 5, 1, 4, 0)
BF = jnp.bfloat16
F32 = jnp.float32


ANY = pl.BlockSpec(memory_space=pl.ANY)
SMEM = pl.BlockSpec(memory_space=pltpu.SMEM)
VMEM = pl.BlockSpec(memory_space=pltpu.VMEM)


def params(mib):
    return pltpu.CompilerParams(vmem_limit_bytes=mib * 1024 * 1024)


def cols(t, width=T):
    return pl.ds(pl.multiple_of(t * width, width), width)


def gather_body(send, z, *outs):
    for o in ORDER:
        for c in range(CAP):
            outs[o][c] = z[:, cols(send[o, c])]


def gather_lists(send_ids, z_state):
    return pl.pallas_call(
        gather_body,
        name="gather_lists",
        out_shape=[jax.ShapeDtypeStruct((CAP, H, T), BF)] * PEERS,
        in_specs=[SMEM, VMEM],
        out_specs=[VMEM] * PEERS,
        compiler_params=params(16),
        cost_estimate=pl.CostEstimate(flops=10**9, transcendentals=0, bytes_accessed=5 * 2**20),
    )(send_ids, z_state)


def tile_copies(v_hbm, v, sems):
    return [
        pltpu.make_async_copy(
            v_hbm.at[pl.ds(i * PER, PER)], v.at[pl.ds(i * PER, PER)], sems.at[i]
        )
        for i in range(CHUNKS)
    ]


def back_body(src, dst, z_hbm, adj_hbm, cot_hbm, w, v_hbm, *rest):
    outs = rest[:PEERS]
    base_hbm, masked_hbm = rest[PEERS : PEERS + 2]
    z, masked, cot, v, back, acc, packed, sems, v_sems, out_sems = rest[PEERS + 2 :]
    load_z = pltpu.make_async_copy(z_hbm, z, sems.at[0])
    load_a = pltpu.make_async_copy(adj_hbm, masked, sems.at[1])
    load_c = pltpu.make_async_copy(cot_hbm, cot, sems.at[2])
    load_v = tile_copies(v_hbm, v, v_sems)
    load_z.start()
    load_a.start()
    load_c.start()
    for copy in load_v:
        copy.start()

    def clear(j, carry):
        acc[LOC + j] = jnp.zeros((H, T), F32)
        return carry

    lax.fori_loop(0, PEERS * CAP, clear, 0, unroll=4)
    load_z.wait()
    load_a.wait()
    wt = w[...]

    def mask(i, carry):
        at = cols(i, 4 * T)
        kept = jnp.where(z[:, at].astype(F32) > 0, masked[:, at].astype(F32), 0.0).astype(BF)
        masked[:, at] = kept
        moved = lax.dot_general(wt, kept, (((0,), (0,)), ((), ())), preferred_element_type=F32)
        moved = moved.astype(BF)
        for j in range(4):
            back[i * 4 + j] = moved[:, j * T : (j + 1) * T]
        return carry

    lax.fori_loop(0, LOC // 4, mask, 0)
    keep = pltpu.make_async_copy(masked, masked_hbm, sems.at[3])
    keep.start()
    load_c.wait()

    def start(t, carry):
        acc[t] = cot[:, cols(t)].astype(F32)
        return carry

    lax.fori_loop(0, LOC, start, 0, unroll=4)
    for i in range(CHUNKS):
        load_v[i].wait()

        def step(g, carry):
            first = i * PER + g * UNROLL
            parts = [
                lax.dot_general(
                    back[dst[first + u]],
                    v[first + u],
                    (((1,), (1,)), ((), ())),
                    preferred_element_type=F32,
                )
                for u in range(UNROLL)
            ]
            for u in range(UNROLL):
                s = src[first + u]
                acc[s] = acc[s] + parts[u]
            return carry

        lax.fori_loop(0, PER // UNROLL, step, 0)
    copies = []
    for n, o in enumerate(ORDER):

        def pack(c, carry):
            packed[o * CAP + c] = acc[LOC + o * CAP + c].astype(BF)
            return carry

        lax.fori_loop(0, CAP, pack, 0, unroll=4)
        copy = pltpu.make_async_copy(packed.at[pl.ds(o * CAP, CAP)], outs[o], out_sems.at[n])
        copy.start()
        copies.append(copy)
    base = pltpu.make_async_copy(acc.at[pl.ds(0, LOC)], base_hbm, sems.at[4])
    base.start()
    for copy in copies:
        copy.wait()
    base.wait()
    keep.wait()


def back_partials(src, dst, z_state, adjoint, cotangent, mix_weight, tile_values):
    outs = pl.pallas_call(
        back_body,
        name="back_partials",
        out_shape=[jax.ShapeDtypeStruct((CAP, H, T), BF)] * PEERS
        + [
            jax.ShapeDtypeStruct((LOC, H, T), F32),
            jax.ShapeDtypeStruct((H, NODES_DEV), BF),
        ],
        in_specs=[SMEM, SMEM, ANY, ANY, ANY, VMEM, ANY],
        out_specs=[ANY] * (PEERS + 2),
        scratch_shapes=[
            pltpu.VMEM((H, NODES_DEV), BF),
            pltpu.VMEM((H, NODES_DEV), BF),
            pltpu.VMEM((H, NODES_DEV), BF),
            pltpu.VMEM((TILES, T, T), BF),
            pltpu.VMEM((LOC, H, T), BF),
            pltpu.VMEM((CODES, H, T), F32),
            pltpu.VMEM((PEERS * CAP, H, T), BF),
            pltpu.SemaphoreType.DMA((5,)),
            pltpu.SemaphoreType.DMA((CHUNKS,)),
            pltpu.SemaphoreType.DMA((PEERS,)),
        ],
        compiler_params=params(44),
        cost_estimate=pl.CostEstimate(
            flops=4 * 10**9, transcendentals=0, bytes_accessed=20 * 2**20
        ),
    )(src, dst, z_state, adjoint, cotangent, mix_weight, tile_values)
    return outs[:PEERS], outs[PEERS], outs[PEERS + 1]


def input_body(masked, inputs, out):
    total = jnp.zeros((H, F), F32)
    width = 8 * T

    def step(i, total):
        at = cols(i, width)
        return total + lax.dot_general(
            masked[:, at], inputs[:, at], (((1,), (1,)), ((), ())), preferred_element_type=F32
        )

    out[...] = lax.fori_loop(0, NODES_DEV // width, step, total)


def input_product(masked, inputs):
    return pl.pallas_call(
        input_body,
        name="input_product",
        out_shape=jax.ShapeDtypeStruct((H, F), F32),
        in_specs=[VMEM, VMEM],
        out_specs=VMEM,
        compiler_params=params(16),
        cost_estimate=pl.CostEstimate(
            flops=10**9, transcendentals=0, bytes_accessed=4 * 2**20
        ),
    )(masked, inputs)


def forward_body(src, dst, z_hbm, x_hbm, m_hbm, w, b, v_hbm, grad, *rest):
    arrived = rest[:PEERS]
    next_hbm, red = rest[PEERS : PEERS + 2]
    z, x, m, v, table, agg, sems, v_sems, in_sems = rest[PEERS + 2 :]
    load_z = pltpu.make_async_copy(z_hbm, z, sems.at[0])
    load_x = pltpu.make_async_copy(x_hbm, x, sems.at[1])
    load_m = pltpu.make_async_copy(m_hbm, m, sems.at[2])
    load_v = tile_copies(v_hbm, v, v_sems)
    halo = [
        pltpu.make_async_copy(
            arrived[o], table.at[pl.ds(LOC + o * CAP, CAP)], in_sems.at[o]
        )
        for o in range(PEERS)
    ]
    load_z.start()
    for copy in halo:
        copy.start()
    for copy in load_v:
        copy.start()
    load_x.start()
    load_m.start()

    def clear(t, carry):
        agg[t] = jnp.zeros((H, T), F32)
        return carry

    lax.fori_loop(0, LOC, clear, 0, unroll=4)
    load_z.wait()

    def local(t, carry):
        table[t] = z[:, cols(t)]
        return carry

    lax.fori_loop(0, LOC, local, 0, unroll=4)
    for copy in halo:
        copy.wait()
    for i in range(CHUNKS):
        load_v[i].wait()

        def step(g, carry):
            first = i * PER + g * UNROLL
            parts = [
                jnp.dot(table[src[first + u]], v[first + u], preferred_element_type=F32)
                for u in range(UNROLL)
            ]
            for u in range(UNROLL):
                d = dst[first + u]
                agg[d] = agg[d] + parts[u]
            return carry

        lax.fori_loop(0, PER // UNROLL, step, 0)
    load_x.wait()
    load_m.wait()
    wt = w[...]
    bt = b[...]

    def finish(i, total):
        at = cols(i, 4 * T)
        a = jnp.concatenate([agg[i * 4 + j].astype(BF) for j in range(4)], axis=1)
        pre = jnp.dot(wt, a, preferred_element_type=F32) + jnp.dot(
            bt, x[:, at], preferred_element_type=F32
        )
        z[:, at] = jnp.maximum(pre, 0.0).astype(BF)
        return total + lax.dot_general(
            m[:, at], a, (((1,), (1,)), ((), ())), preferred_element_type=F32
        )

    total = lax.fori_loop(0, LOC // 4, finish, jnp.zeros((H, H), F32))
    store = pltpu.make_async_copy(z, next_hbm, sems.at[0])
    store.start()
    scale = 1.0 / math.sqrt(NODES_DEV * 128)
    red[:, :F] = grad[...] * scale
    red[:, F : F + H] = total * scale
    red[:, F + H :] = jnp.zeros((H, 2 * T - F - H), F32)
    store.wait()


def forward(src, dst, z_state, inputs, masked, mix_weight, input_weight, tile_values, grad, lists):
    return pl.pallas_call(
        forward_body,
        name="forward",
        out_shape=[
            jax.ShapeDtypeStruct((H, NODES_DEV), BF),
            jax.ShapeDtypeStruct((H, 2 * T), F32),
        ],
        in_specs=[SMEM, SMEM, ANY, ANY, ANY, VMEM, VMEM, ANY, VMEM] + [ANY] * PEERS,
        out_specs=[ANY, VMEM],
        scratch_shapes=[
            pltpu.VMEM((H, NODES_DEV), BF),
            pltpu.VMEM((F, NODES_DEV), BF),
            pltpu.VMEM((H, NODES_DEV), BF),
            pltpu.VMEM((TILES, T, T), BF),
            pltpu.VMEM((CODES, H, T), BF),
            pltpu.VMEM((LOC, H, T), F32),
            pltpu.SemaphoreType.DMA((3,)),
            pltpu.SemaphoreType.DMA((CHUNKS,)),
            pltpu.SemaphoreType.DMA((PEERS,)),
        ],
        compiler_params=params(44),
        cost_estimate=pl.CostEstimate(
            flops=4 * 10**9, transcendentals=0, bytes_accessed=20 * 2**20
        ),
    )(src, dst, z_state, inputs, masked, mix_weight, input_weight, tile_values, grad, *lists)


def finish_body(send, base_hbm, *rest):
    lists = rest[:PEERS]
    out = rest[PEERS]
    acc, parts, sem, in_sems = rest[PEERS + 1 :]
    load = pltpu.make_async_copy(base_hbm, acc, sem.at[0])
    load.start()
    copies = [
        pltpu.make_async_copy(lists[o], parts.at[pl.ds(o * CAP, CAP)], in_sems.at[o])
        for o in range(PEERS)
    ]
    for copy in copies:
        copy.start()
    load.wait()
    for o in range(PEERS):
        copies[o].wait()
        for c in range(CAP):
            t = send[o, c]
            acc[t] = acc[t] + parts[o * CAP + c].astype(F32)
    for t in range(LOC):
        out[:, t * T : (t + 1) * T] = acc[t].astype(BF)


def finish_adjoint(send_ids, base, lists):
    return pl.pallas_call(
        finish_body,
        name="finish_adjoint",
        out_shape=jax.ShapeDtypeStruct((H, NODES_DEV), BF),
        in_specs=[SMEM, ANY] + [ANY] * PEERS,
        out_specs=VMEM,
        scratch_shapes=[
            pltpu.VMEM((LOC, H, T), F32),
            pltpu.VMEM((PEERS * CAP, H, T), BF),
            pltpu.SemaphoreType.DMA((1,)),
            pltpu.SemaphoreType.DMA((PEERS,)),
        ],
        compiler_params=params(24),
        cost_estimate=pl.CostEstimate(
            flops=10**9, transcendentals=0, bytes_accessed=8 * 2**20
        ),
    )(send_ids, base, *lists)


def shift(array, by):
    n = lax.axis_size(AXIS)
    return lax.ppermute(array, AXIS, [(i, (i + by) % n) for i in range(n)])


def swap(array, bits):
    n = lax.axis_size(AXIS)
    return lax.ppermute(array, AXIS, [(i, i ^ bits) for i in range(n)])


def summed(total):
    for low in (5, 3, 1):
        one, two, three = (swap(total, k << low) for k in (1, 2, 3))
        total = (total + one) + (two + three)
    return total + swap(total, 1)


def exchange(lists, sign):
    got = [None] * PEERS
    for o in ORDER:
        got[o] = shift(lists[o], sign * OFFSETS[o])
    return got


def per_device(
    z_state,
    inputs,
    adjoint,
    cotangent,
    mix_weight,
    input_weight,
    tile_values,
    tile_src,
    tile_dst,
    send_list,
):
    src, dst, send_ids = tile_src[0], tile_dst[0], send_list[0]
    arrived = exchange(gather_lists(send_ids, z_state), 1)
    leaving, base, masked = back_partials(
        src, dst, z_state, adjoint, cotangent, mix_weight, tile_values
    )
    returned = exchange(leaving, -1)
    grad = input_product(masked, inputs)
    fixed_next, red = forward(
        src, dst, z_state, inputs, masked, mix_weight, input_weight, tile_values, grad,
        arrived,
    )
    total = summed(red)
    adjoint_next = finish_adjoint(send_ids, base, returned)
    return fixed_next, adjoint_next, total[:, F : F + H], total[:, :F]


def solution(mesh):
    dom = P(None, AXIS)
    return jax.shard_map(
        per_device,
        mesh=mesh,
        in_specs=(
            dom,
            dom,
            dom,
            dom,
            P(),
            P(),
            P(AXIS, None, None),
            P(AXIS, None),
            P(AXIS, None),
            P(AXIS, None, None),
        ),
        out_specs=(dom, dom, P(), P()),
        check_vma=False,
    )
```

```python
import math

import jax
import jax.numpy as jnp
from jax import lax
from jax.experimental import pallas as pl
from jax.experimental.pallas import tpu as pltpu
from jax.sharding import PartitionSpec as P


AXIS = "dom"
H = 96
F = 128
T = 128
LOC = 64
CAP = 16
PEERS = 8
TILES = 256
NODES_DEV = LOC * T
CODES = LOC + PEERS * CAP
CHUNKS = 4
PER = TILES // CHUNKS
UNROLL = 32
OFFSETS = (1, 2, 3, 4, -1, -2, -3, -4)
ORDER = (3, 7, 6, 5, 4, 2, 1, 0)
HOME = (1, 0, 5, 4, 3, 2, 7, 6)
BF = jnp.bfloat16
F32 = jnp.float32


SMEM = pl.BlockSpec(memory_space=pltpu.SMEM)
VMEM = pl.BlockSpec(memory_space=pltpu.VMEM)
HBM = pl.BlockSpec(memory_space=pltpu.HBM)
LISTS = [jax.ShapeDtypeStruct((CAP, H, T), BF)] * PEERS


def params(mib):
    return pltpu.CompilerParams(vmem_limit_bytes=mib * 1024 * 1024)


def cost(gflops, mib):
    return pl.CostEstimate(
        flops=int(gflops * 10**9), transcendentals=0, bytes_accessed=mib * 2**20
    )


def hbm(array):
    return pltpu.with_memory_space_constraint(array, pltpu.HBM)


def cols(t, width=T):
    return pl.ds(pl.multiple_of(t * width, width), width)


def gather_body(send_hbm, z_hbm, *rest):
    outs = rest[:PEERS]
    send, z, sems = rest[PEERS:]
    load_z = pltpu.make_async_copy(z_hbm, z, sems.at[0])
    load_s = pltpu.make_async_copy(send_hbm, send, sems.at[1])
    load_z.start()
    load_s.start()
    load_s.wait()
    load_z.wait()
    for o in ORDER:
        for c in range(CAP):
            outs[o][c] = z[:, cols(send[0, o, c])]


def gather_lists(send_list, z_state):
    return pl.pallas_call(
        gather_body,
        name="gather_lists",
        out_shape=LISTS,
        in_specs=[HBM, HBM],
        out_specs=[VMEM] * PEERS,
        scratch_shapes=[
            pltpu.SMEM((1, PEERS, CAP), jnp.int32),
            pltpu.VMEM((H, NODES_DEV), BF),
            pltpu.SemaphoreType.DMA((2,)),
        ],
        compiler_params=params(6),
        cost_estimate=cost(1, 5),
    )(hbm(send_list), hbm(z_state))


def back_body(src, dst, z, adj, cot_hbm, w, v_hbm, *rest):
    outs = rest[:PEERS]
    acc, masked, v, back, cot, sem, v_sems = rest[PEERS:]
    load_c = pltpu.make_async_copy(cot_hbm, cot, sem.at[0])
    load_v = [
        pltpu.make_async_copy(
            v_hbm.at[pl.ds(i * PER, PER)], v.at[pl.ds(i * PER, PER)], v_sems.at[i]
        )
        for i in range(CHUNKS)
    ]
    load_c.start()
    for copy in load_v:
        copy.start()

    def clear(j, carry):
        acc[LOC + j] = jnp.zeros((H, T), F32)
        return carry

    lax.fori_loop(0, PEERS * CAP, clear, 0, unroll=4)
    wt = w[...]

    def mask(i, carry):
        at = cols(i, 4 * T)
        kept = jnp.where(z[:, at].astype(F32) > 0, adj[:, at].astype(F32), 0.0).astype(BF)
        masked[:, at] = kept
        moved = lax.dot_general(wt, kept, (((0,), (0,)), ((), ())), preferred_element_type=F32)
        moved = moved.astype(BF)
        for j in range(4):
            back[i * 4 + j] = moved[:, j * T : (j + 1) * T]
        return carry

    lax.fori_loop(0, LOC // 4, mask, 0)
    load_c.wait()

    def own(t, carry):
        acc[t] = cot[:, cols(t)].astype(F32)
        return carry

    lax.fori_loop(0, LOC, own, 0, unroll=4)

    def step(g, carry):
        first = g * UNROLL
        parts = [
            lax.dot_general(
                back[dst[0, first + u]],
                v[first + u],
                (((1,), (1,)), ((), ())),
                preferred_element_type=F32,
            )
            for u in range(UNROLL)
        ]
        for u in range(UNROLL):
            s = src[0, first + u]
            acc[s] = acc[s] + parts[u]
        return carry

    for i in range(CHUNKS):
        load_v[i].wait()
        lax.fori_loop(i * PER // UNROLL, (i + 1) * PER // UNROLL, step, 0)
    for o in range(PEERS):

        def pack(c, carry):
            outs[o][c] = acc[LOC + o * CAP + c].astype(BF)
            return carry

        lax.fori_loop(0, CAP, pack, 0, unroll=4)


def back_partials(src, dst, z_state, adjoint, cotangent, mix_weight, tile_values):
    outs = pl.pallas_call(
        back_body,
        name="back_partials",
        out_shape=LISTS
        + [
            jax.ShapeDtypeStruct((CODES, H, T), F32),
            jax.ShapeDtypeStruct((H, NODES_DEV), BF),
            jax.ShapeDtypeStruct((TILES, T, T), BF),
        ],
        in_specs=[SMEM, SMEM, VMEM, VMEM, HBM, VMEM, HBM],
        out_specs=[VMEM] * (PEERS + 3),
        scratch_shapes=[
            pltpu.VMEM((LOC, H, T), BF),
            pltpu.VMEM((H, NODES_DEV), BF),
            pltpu.SemaphoreType.DMA((1,)),
            pltpu.SemaphoreType.DMA((CHUNKS,)),
        ],
        compiler_params=params(8),
        cost_estimate=cost(4, 20),
    )(src, dst, z_state, adjoint, hbm(cotangent), mix_weight, hbm(tile_values))
    return outs[:PEERS], outs[PEERS:]


def input_body(masked, inputs, out):
    width = 8 * T

    def step(i, total):
        at = cols(i, width)
        return total + lax.dot_general(
            masked[:, at], inputs[:, at], (((1,), (1,)), ((), ())), preferred_element_type=F32
        )

    out[...] = lax.fori_loop(0, NODES_DEV // width, step, jnp.zeros((H, F), F32))


def input_product(masked, inputs):
    return pl.pallas_call(
        input_body,
        name="input_product",
        out_shape=jax.ShapeDtypeStruct((H, F), F32),
        in_specs=[VMEM, VMEM],
        out_specs=VMEM,
        compiler_params=params(12),
        cost_estimate=cost(1, 4),
    )(masked, inputs)


def forward_body(src, dst, z, m, v, grad, *rest):
    arrived = rest[:PEERS]
    out, keep, give = rest[PEERS : PEERS + 3]
    table, agg = rest[PEERS + 3 :]

    def local(t, carry):
        table[t] = z[:, cols(t)]
        agg[t] = jnp.zeros((H, T), F32)
        return carry

    lax.fori_loop(0, LOC, local, 0, unroll=4)
    for o in range(PEERS):

        def halo(c, carry):
            table[LOC + o * CAP + c] = arrived[o][c]
            return carry

        lax.fori_loop(0, CAP, halo, 0, unroll=4)

    def step(g, carry):
        first = g * UNROLL
        parts = [
            jnp.dot(table[src[0, first + u]], v[first + u], preferred_element_type=F32)
            for u in range(UNROLL)
        ]
        for u in range(UNROLL):
            d = dst[0, first + u]
            agg[d] = agg[d] + parts[u]
        return carry

    lax.fori_loop(0, TILES // UNROLL, step, 0)

    def finish(i, total):
        at = cols(i, 4 * T)
        a = jnp.concatenate([agg[i * 4 + j].astype(BF) for j in range(4)], axis=1)
        out[:, at] = a
        return total + lax.dot_general(
            m[:, at], a, (((1,), (1,)), ((), ())), preferred_element_type=F32
        )

    total = lax.fori_loop(0, LOC // 4, finish, jnp.zeros((H, H), F32))
    scale = 1.0 / math.sqrt(NODES_DEV * 128)
    inner = grad[...] * scale
    weight = jnp.concatenate([total * scale, jnp.zeros((H, F - H), F32)], axis=1)
    first = lax.rem(lax.axis_index(AXIS), 2) == 0
    keep[...] = jnp.where(first, inner, weight)
    give[...] = jnp.where(first, weight, inner)


def forward(src, dst, z_state, masked, tile_values, grad, lists):
    return pl.pallas_call(
        forward_body,
        name="forward",
        out_shape=[
            jax.ShapeDtypeStruct((H, NODES_DEV), BF),
            jax.ShapeDtypeStruct((H, F), F32),
            jax.ShapeDtypeStruct((H, F), F32),
        ],
        in_specs=[SMEM, SMEM] + [VMEM] * (4 + PEERS),
        out_specs=[VMEM] * 3,
        scratch_shapes=[pltpu.VMEM((CODES, H, T), BF), pltpu.VMEM((LOC, H, T), F32)],
        compiler_params=params(12),
        cost_estimate=cost(3, 15),
    )(src, dst, z_state, masked, tile_values, grad, *lists)


def mix_body(a, x, w, b, out):
    wt = w[...]
    bt = b[...]

    def step(i, carry):
        at = cols(i, 4 * T)
        pre = jnp.dot(wt, a[:, at], preferred_element_type=F32) + jnp.dot(
            bt, x[:, at], preferred_element_type=F32
        )
        out[:, at] = jnp.maximum(pre, 0.0).astype(BF)
        return carry

    lax.fori_loop(0, LOC // 4, step, 0)


def mixed(aggregated, inputs, mix_weight, input_weight):
    return pl.pallas_call(
        mix_body,
        name="mixed",
        out_shape=jax.ShapeDtypeStruct((H, NODES_DEV), BF),
        in_specs=[VMEM] * 4,
        out_specs=VMEM,
        compiler_params=params(12),
        cost_estimate=cost(1, 5),
    )(aggregated, inputs, mix_weight, input_weight)


def finish_body(send, given, *rest):
    lists = rest[:PEERS]
    out, acc = rest[PEERS:]
    for o in range(PEERS):
        for c in range(CAP):
            t = send[0, o, c]
            acc[t] = acc[t] + lists[o][c].astype(F32)
    for t in range(LOC):
        out[:, t * T : (t + 1) * T] = acc[t].astype(BF)


def finish_adjoint(send_list, acc, lists):
    return pl.pallas_call(
        finish_body,
        name="finish_adjoint",
        out_shape=[
            jax.ShapeDtypeStruct((H, NODES_DEV), BF),
            jax.ShapeDtypeStruct((CODES, H, T), F32),
        ],
        in_specs=[SMEM] + [VMEM] * (1 + PEERS),
        out_specs=[VMEM] * 2,
        input_output_aliases={1: 1},
        compiler_params=params(8),
        cost_estimate=cost(1, 8),
    )(send_list, acc, *lists)[0]


def ending_body(mine, theirs, weight, inner):
    first = lax.rem(lax.axis_index(AXIS), 2) == 0
    inner[...] = jnp.where(first, mine[...], theirs[...])
    weight[...] = jnp.where(first, theirs[:, :H], mine[:, :H])


def ending(mine, theirs):
    return pl.pallas_call(
        ending_body,
        name="ending",
        out_shape=[jax.ShapeDtypeStruct((H, H), F32), jax.ShapeDtypeStruct((H, F), F32)],
        in_specs=[VMEM, VMEM],
        out_specs=[VMEM] * 2,
        compiler_params=params(4),
    )(mine, theirs)


def shift(array, by):
    n = lax.axis_size(AXIS)
    return lax.ppermute(array, AXIS, [(i, (i + by) % n) for i in range(n)])


def swap(array, bits):
    n = lax.axis_size(AXIS)
    return lax.ppermute(array, AXIS, [(i, i ^ bits) for i in range(n)])


def quads(total):
    for low in (5, 3, 1):
        one, two, three = (swap(total, k << low) for k in (1, 2, 3))
        total = (total + one) + (two + three)
    return total


def exchange(lists, sign, order):
    got = [None] * PEERS
    for o in order:
        got[o] = shift(lists[o], sign * OFFSETS[o])
    return got


def per_device(
    z_state,
    inputs,
    adjoint,
    cotangent,
    mix_weight,
    input_weight,
    tile_values,
    tile_src,
    tile_dst,
    send_list,
):
    arrived = exchange(gather_lists(send_list, z_state), 1, ORDER)
    leaving, (acc, masked, held) = back_partials(
        tile_src, tile_dst, z_state, adjoint, cotangent, mix_weight, tile_values
    )
    returned = exchange(leaving, -1, HOME)
    grad = input_product(masked, inputs)
    aggregated, keep, give = forward(
        tile_src, tile_dst, z_state, masked, held, grad, arrived
    )
    total = keep + swap(give, 1)
    total = quads(total)
    fixed_next = mixed(aggregated, inputs, mix_weight, input_weight)
    adjoint_next = finish_adjoint(send_list, acc, returned)
    other = swap(total, 1)
    weight, inner = ending(total, other)
    return fixed_next, adjoint_next, weight, inner


def solution(mesh):
    dom = P(None, AXIS)
    return jax.shard_map(
        per_device,
        mesh=mesh,
        in_specs=(
            dom,
            dom,
            dom,
            dom,
            P(),
            P(),
            P(AXIS, None, None),
            P(AXIS, None),
            P(AXIS, None),
            P(AXIS, None, None),
        ),
        out_specs=(dom, dom, P(), P()),
        check_vma=False,
    )
```

```python
import math

import jax
import jax.numpy as jnp
from jax import lax
from jax.experimental import pallas as pl
from jax.experimental.pallas import tpu as pltpu
from jax.sharding import PartitionSpec as P


AXIS = "dom"
H = 96
F = 128
T = 128
LOC = 64
CAP = 16
PEERS = 8
TILES = 256
NODES_DEV = LOC * T
CODES = LOC + PEERS * CAP
CHUNKS = 4
PER = TILES // CHUNKS
UNROLL = 64
WIDE = 32
STEPS = ((3, 1), (2, 2), (1, 3), (4, 4), (-1, -3), (-2, -2), (-3, -1), (-4, -4))
OWNER = ((2, 0), (1, 1), (0, 2), (3, 3), (4, 6), (5, 5), (6, 4), (7, 7))
ORDER = (3, 7, 6, 2, 1, 0, 5, 4)
HOME = (1, 0, 5, 4, 3, 7, 6, 2)
BF = jnp.bfloat16
F32 = jnp.float32


SMEM = pl.BlockSpec(memory_space=pltpu.SMEM)
VMEM = pl.BlockSpec(memory_space=pltpu.VMEM)
HBM = pl.BlockSpec(memory_space=pltpu.HBM)
LISTS = [jax.ShapeDtypeStruct((CAP, H, T), BF)] * PEERS


def params(mib):
    return pltpu.CompilerParams(vmem_limit_bytes=mib * 1024 * 1024)


def cost(gflops, mib):
    return pl.CostEstimate(
        flops=int(gflops * 10**9), transcendentals=0, bytes_accessed=mib * 2**20
    )


def hbm(array):
    return pltpu.with_memory_space_constraint(array, pltpu.HBM)


def listed(channel, reader):
    even, odd = OWNER[channel]
    if even == odd:
        return even
    side = lax.rem(lax.axis_index(AXIS) + reader, 2)
    return jnp.where(side == 0, even, odd)


def cols(t, width=T):
    return pl.ds(pl.multiple_of(t * width, width), width)


def gather_body(send_hbm, z_hbm, *rest):
    outs = rest[:PEERS]
    send, z, sems = rest[PEERS:]
    load_z = pltpu.make_async_copy(z_hbm, z, sems.at[0])
    load_s = pltpu.make_async_copy(send_hbm, send, sems.at[1])
    load_z.start()
    load_s.start()
    load_s.wait()
    load_z.wait()
    for ch in ORDER:
        o = listed(ch, 0)
        for c in range(CAP):
            outs[ch][c] = z[:, cols(send[0, o, c])]


def gather_lists(send_list, z_state):
    return pl.pallas_call(
        gather_body,
        name="gather_lists",
        out_shape=LISTS,
        in_specs=[HBM, HBM],
        out_specs=[VMEM] * PEERS,
        scratch_shapes=[
            pltpu.SMEM((1, PEERS, CAP), jnp.int32),
            pltpu.VMEM((H, NODES_DEV), BF),
            pltpu.SemaphoreType.DMA((2,)),
        ],
        compiler_params=params(6),
        cost_estimate=cost(1, 5),
    )(hbm(send_list), hbm(z_state))


def back_body(src, dst, z, adj, cot_hbm, w, v_hbm, *rest):
    outs = rest[:PEERS]
    acc, masked, v, back, cot, sem, v_sems = rest[PEERS:]
    load_c = pltpu.make_async_copy(cot_hbm, cot, sem.at[0])
    load_v = [
        pltpu.make_async_copy(
            v_hbm.at[pl.ds(i * PER, PER)], v.at[pl.ds(i * PER, PER)], v_sems.at[i]
        )
        for i in range(CHUNKS)
    ]
    load_c.start()
    for copy in load_v:
        copy.start()

    def clear(j, carry):
        acc[LOC + j] = jnp.zeros((H, T), F32)
        return carry

    lax.fori_loop(0, PEERS * CAP, clear, 0, unroll=4)
    wt = w[...]

    def mask(i, carry):
        at = cols(i, WIDE * T)
        kept = jnp.where(z[:, at].astype(F32) > 0, adj[:, at].astype(F32), 0.0).astype(BF)
        masked[:, at] = kept
        moved = lax.dot_general(wt, kept, (((0,), (0,)), ((), ())), preferred_element_type=F32)
        moved = moved.astype(BF)
        for j in range(WIDE):
            back[i * WIDE + j] = moved[:, j * T : (j + 1) * T]
        return carry

    lax.fori_loop(0, LOC // WIDE, mask, 0)
    load_c.wait()

    def own(t, carry):
        acc[t] = cot[:, cols(t)].astype(F32)
        return carry

    lax.fori_loop(0, LOC, own, 0, unroll=4)

    def step(g, carry):
        first = g * UNROLL
        parts = [
            lax.dot_general(
                back[dst[0, first + u]],
                v[first + u],
                (((1,), (1,)), ((), ())),
                preferred_element_type=F32,
            )
            for u in range(UNROLL)
        ]
        for u in range(UNROLL):
            s = src[0, first + u]
            acc[s] = acc[s] + parts[u]
        return carry

    for i in range(CHUNKS):
        load_v[i].wait()
        lax.fori_loop(i * PER // UNROLL, (i + 1) * PER // UNROLL, step, 0)
    for ch in range(PEERS):
        first = LOC + listed(ch, 1) * CAP

        def pack(c, carry):
            outs[ch][c] = acc[first + c].astype(BF)
            return carry

        lax.fori_loop(0, CAP, pack, 0, unroll=4)


def back_partials(src, dst, z_state, adjoint, cotangent, mix_weight, tile_values):
    outs = pl.pallas_call(
        back_body,
        name="back_partials",
        out_shape=LISTS
        + [
            jax.ShapeDtypeStruct((CODES, H, T), F32),
            jax.ShapeDtypeStruct((H, NODES_DEV), BF),
            jax.ShapeDtypeStruct((TILES, T, T), BF),
        ],
        in_specs=[SMEM, SMEM, VMEM, VMEM, HBM, VMEM, HBM],
        out_specs=[VMEM] * (PEERS + 3),
        scratch_shapes=[
            pltpu.VMEM((LOC, H, T), BF),
            pltpu.VMEM((H, NODES_DEV), BF),
            pltpu.SemaphoreType.DMA((1,)),
            pltpu.SemaphoreType.DMA((CHUNKS,)),
        ],
        compiler_params=params(8),
        cost_estimate=cost(4, 20),
    )(src, dst, z_state, adjoint, hbm(cotangent), mix_weight, hbm(tile_values))
    return outs[:PEERS], outs[PEERS:]


def input_body(masked, inputs, out):
    width = 8 * T

    def step(i, total):
        at = cols(i, width)
        return total + lax.dot_general(
            masked[:, at], inputs[:, at], (((1,), (1,)), ((), ())), preferred_element_type=F32
        )

    out[...] = lax.fori_loop(0, NODES_DEV // width, step, jnp.zeros((H, F), F32))


def input_product(masked, inputs):
    return pl.pallas_call(
        input_body,
        name="input_product",
        out_shape=jax.ShapeDtypeStruct((H, F), F32),
        in_specs=[VMEM, VMEM],
        out_specs=VMEM,
        compiler_params=params(12),
        cost_estimate=cost(1, 4),
    )(masked, inputs)


def forward_body(src, dst, z, m, v, grad, *rest):
    arrived = rest[:PEERS]
    out, keep, give = rest[PEERS : PEERS + 3]
    table, agg = rest[PEERS + 3 :]

    def local(t, carry):
        table[t] = z[:, cols(t)]
        agg[t] = jnp.zeros((H, T), F32)
        return carry

    lax.fori_loop(0, LOC, local, 0, unroll=4)
    for ch in range(PEERS):
        place = LOC + listed(ch, 1) * CAP

        def halo(c, carry):
            table[place + c] = arrived[ch][c]
            return carry

        lax.fori_loop(0, CAP, halo, 0, unroll=4)

    def step(g, carry):
        first = g * UNROLL
        parts = [
            jnp.dot(table[src[0, first + u]], v[first + u], preferred_element_type=F32)
            for u in range(UNROLL)
        ]
        for u in range(UNROLL):
            d = dst[0, first + u]
            agg[d] = agg[d] + parts[u]
        return carry

    lax.fori_loop(0, TILES // UNROLL, step, 0)

    def finish(i, total):
        at = cols(i, WIDE * T)
        a = jnp.concatenate([agg[i * WIDE + j].astype(BF) for j in range(WIDE)], axis=1)
        out[:, at] = a
        return total + lax.dot_general(
            m[:, at], a, (((1,), (1,)), ((), ())), preferred_element_type=F32
        )

    total = lax.fori_loop(0, LOC // WIDE, finish, jnp.zeros((H, H), F32))
    scale = 1.0 / math.sqrt(NODES_DEV * 128)
    inner = grad[...] * scale
    weight = jnp.concatenate([total * scale, jnp.zeros((H, F - H), F32)], axis=1)
    first = lax.rem(lax.axis_index(AXIS), 2) == 0
    keep[...] = jnp.where(first, inner, weight)
    give[...] = jnp.where(first, weight, inner)


def forward(src, dst, z_state, masked, tile_values, grad, lists):
    return pl.pallas_call(
        forward_body,
        name="forward",
        out_shape=[
            jax.ShapeDtypeStruct((H, NODES_DEV), BF),
            jax.ShapeDtypeStruct((H, F), F32),
            jax.ShapeDtypeStruct((H, F), F32),
        ],
        in_specs=[SMEM, SMEM] + [VMEM] * (4 + PEERS),
        out_specs=[VMEM] * 3,
        scratch_shapes=[pltpu.VMEM((CODES, H, T), BF), pltpu.VMEM((LOC, H, T), F32)],
        compiler_params=params(12),
        cost_estimate=cost(3, 15),
    )(src, dst, z_state, masked, tile_values, grad, *lists)


def mix_body(a, x, w, b, out):
    wt = w[...]
    bt = b[...]

    def step(i, carry):
        at = cols(i, WIDE * T)
        pre = jnp.dot(wt, a[:, at], preferred_element_type=F32) + jnp.dot(
            bt, x[:, at], preferred_element_type=F32
        )
        out[:, at] = jnp.maximum(pre, 0.0).astype(BF)
        return carry

    lax.fori_loop(0, LOC // WIDE, step, 0)


def mixed(aggregated, inputs, mix_weight, input_weight):
    return pl.pallas_call(
        mix_body,
        name="mixed",
        out_shape=jax.ShapeDtypeStruct((H, NODES_DEV), BF),
        in_specs=[VMEM] * 4,
        out_specs=VMEM,
        compiler_params=params(12),
        cost_estimate=cost(1, 5),
    )(aggregated, inputs, mix_weight, input_weight)


LIGHT = (0, 1, 4, 5)
HEAVY = (2, 3, 6, 7)


def settle(which, send, acc, lists):
    for ch, part in zip(which, lists):
        o = listed(ch, 0)
        for c in range(CAP):
            t = send[0, o, c]
            acc[t] = acc[t] + part[c].astype(F32)


def early_body(send, given, *rest):
    settle(LIGHT, send, rest[-1], rest[:-1])


def finish_body(send, given, *rest):
    out, acc = rest[-2:]
    settle(HEAVY, send, acc, rest[:-2])
    for t in range(LOC):
        out[:, t * T : (t + 1) * T] = acc[t].astype(BF)


def settle_light(send_list, acc, lists):
    return pl.pallas_call(
        early_body,
        name="settle_light",
        out_shape=jax.ShapeDtypeStruct((CODES, H, T), F32),
        in_specs=[SMEM] + [VMEM] * (1 + len(LIGHT)),
        out_specs=VMEM,
        input_output_aliases={1: 0},
        compiler_params=params(8),
        cost_estimate=cost(0.4, 3),
    )(send_list, acc, *(lists[o] for o in LIGHT))


def finish_adjoint(send_list, acc, lists):
    return pl.pallas_call(
        finish_body,
        name="finish_adjoint",
        out_shape=[
            jax.ShapeDtypeStruct((H, NODES_DEV), BF),
            jax.ShapeDtypeStruct((CODES, H, T), F32),
        ],
        in_specs=[SMEM] + [VMEM] * (1 + len(HEAVY)),
        out_specs=[VMEM] * 2,
        input_output_aliases={1: 1},
        compiler_params=params(8),
        cost_estimate=cost(0.6, 5),
    )(send_list, acc, *(lists[o] for o in HEAVY))[0]


def ending_body(mine, theirs, weight, inner):
    first = lax.rem(lax.axis_index(AXIS), 2) == 0
    inner[...] = jnp.where(first, mine[...], theirs[...])
    weight[...] = jnp.where(first, theirs[:, :H], mine[:, :H])


def ending(mine, theirs):
    return pl.pallas_call(
        ending_body,
        name="ending",
        out_shape=[jax.ShapeDtypeStruct((H, H), F32), jax.ShapeDtypeStruct((H, F), F32)],
        in_specs=[VMEM, VMEM],
        out_specs=[VMEM] * 2,
        compiler_params=params(4),
    )(mine, theirs)


def shift(array, channel, home):
    n = lax.axis_size(AXIS)
    pairs = [(i, (i + STEPS[channel][i % 2]) % n) for i in range(n)]
    return lax.ppermute(array, AXIS, [(b, a) for a, b in pairs] if home else pairs)


def swap(array, bits):
    n = lax.axis_size(AXIS)
    return lax.ppermute(array, AXIS, [(i, i ^ bits) for i in range(n)])


def quads(total):
    for low in (5, 3, 1):
        one, two, three = (swap(total, k << low) for k in (1, 2, 3))
        total = (total + one) + (two + three)
    return total


def exchange(lists, home, order):
    got = [None] * PEERS
    for o in order:
        got[o] = shift(lists[o], o, home)
    return got


def per_device(
    z_state,
    inputs,
    adjoint,
    cotangent,
    mix_weight,
    input_weight,
    tile_values,
    tile_src,
    tile_dst,
    send_list,
):
    arrived = exchange(gather_lists(send_list, z_state), False, ORDER)
    leaving, (acc, masked, held) = back_partials(
        tile_src, tile_dst, z_state, adjoint, cotangent, mix_weight, tile_values
    )
    returned = exchange(leaving, True, HOME)
    grad = input_product(masked, inputs)
    aggregated, keep, give = forward(
        tile_src, tile_dst, z_state, masked, held, grad, arrived
    )
    total = keep + swap(give, 1)
    total = quads(total)
    fixed_next = mixed(aggregated, inputs, mix_weight, input_weight)
    acc = settle_light(send_list, acc, returned)
    other = swap(total, 1)
    weight, inner = ending(total, other)
    adjoint_next = finish_adjoint(send_list, acc, returned)
    return fixed_next, adjoint_next, weight, inner


def solution(mesh):
    dom = P(None, AXIS)
    return jax.shard_map(
        per_device,
        mesh=mesh,
        in_specs=(
            dom,
            dom,
            dom,
            dom,
            P(),
            P(),
            P(AXIS, None, None),
            P(AXIS, None),
            P(AXIS, None),
            P(AXIS, None, None),
        ),
        out_specs=(dom, dom, P(), P()),
        check_vma=False,
    )
```
